256 devices in a mesh: groups: 2 (over y), expert: 64 (over z, x), tensor: 2 (over core).
Axes of the slice: x: 4, y: 2, z: 16, core: 2. Of those that a mesh axis runs over, the one named last changes fastest.
The devices are a block of a 4x16x16 slice.
Arguments:
- tokens: bfloat16 [32768, 1440], P(('groups', 'expert')), parts along dimension 0, may hold values from -6 to 6
- routes: int32 [32768, 4], P(('groups', 'expert')), parts along dimension 0, may hold values from 0 to 63, all different within a row; in each aligned block of 256 rows (0 to 255, 256 to 511, ...) at most 24 rows name the same one
- gates: float32 [32768, 4], P(('groups', 'expert')), parts along dimension 0, may hold values from 0.1 to 1
- w_gate: bfloat16 [64, 1440, 1440], P('expert', None, 'tensor'), may hold values from -0.15625 to 0.15625
- w_up: bfloat16 [64, 1440, 1440], P('expert', None, 'tensor'), may hold values from -0.15625 to 0.15625
- w_down: bfloat16 [64, 1440, 1440], P('expert', 'tensor'), may hold values from -0.15625 to 0.15625
- shared_gate: bfloat16 [1440, 1440], P(None, 'tensor'), may hold values from -0.15625 to 0.15625
- shared_up: bfloat16 [1440, 1440], P(None, 'tensor'), may hold values from -0.15625 to 0.15625
- shared_down: bfloat16 [1440, 1440], P('tensor'), may hold values from -0.15625 to 0.15625
Outputs:
- mixed: bfloat16 [32768, 1440], P(('groups', 'expert'), 'tensor'), parts along dimension 0
The draws below stay inside these ranges and needn't reach their ends.
There are 2 independent parts, one for each index of `groups`. The reference program is written for one: setup_inputs(seed, part) draws one part's arguments, and reference() takes and returns one part's arrays. A program takes and returns all parts, laid end to end along the dimension named above; an argument that names none is the same for every part. Nothing has to cross between parts.
Inputs may be any that keep to these rules, and one draw needn't show every extreme that they name: `routes`: each token names 4 different experts. Among the 256 tokens of one index of expert (aligned blocks of rows), no expert is named by more than 24 tokens; in some blocks one expert is named by exactly 24.
All inputs are finite; a program needn't handle non-finite values.
Results may differ from the reference program's by a relative error of at most 0.0051.
Values may be sent and summed in bfloat16 or wider, within the bound.
No kernel may reach another device: no remote copies, remote signals or barrier semaphores. Data moves between devices by JAX's collectives and lax.ppermute only.
A program may use at most 192 MiB of HBM per device.

```python
import math
import jax
import jax.numpy as jnp
import numpy as np
from jax import lax

D = 1440
FF = 1440
FS = 1440
TOP = 4
TOK_DEV = 256
EXPERTS = 64
TOKENS = 16384
CAP = 24
N_EXPERT = 64


def levels(stream_key, dims, cuts, least, high):
    level, own = 1.0, jax.random.fold_in(stream_key, 6)
    for dim, blocks in cuts:
        heights = jnp.exp(jax.random.uniform(jax.random.fold_in(own, dim), (blocks,), jnp.float32, least / len(cuts), high / len(cuts)))
        level = level * jnp.repeat(heights, dims[dim] // blocks).reshape([-1 if axis == dim else 1 for axis in range(len(dims))])
    return level


def deal_out(stream_key, own, number, rows, count, top, bound, slope):
    ranking = jax.random.permutation(stream_key, count)
    crowded, usual = shares(count, rows * top, bound, slope, True), shares(count, rows * top, bound, slope, False)
    places = jnp.arange(count)

    def named(tallies, turn):
        used = int((tallies > 0).sum())
        fixed = max(1, used // 4)
        shifted = fixed + (places - fixed + turn * (used - fixed)) % max(1, count - fixed)
        return jnp.zeros((count,), jnp.int32).at[ranking[jnp.where(places < fixed, places, shifted)]].set(jnp.asarray(tallies, jnp.int32))

    tallies = jnp.where(number % 4 == 0, named(crowded, number // 4), named(usual, number - number // 4 - 1))
    mixed = jax.random.permutation(jax.random.fold_in(own, 3), count)
    source_of, receiver = mixed[0:count // 2 * 2:2], mixed[1:count // 2 * 2:2]
    margin = jnp.minimum(tallies[source_of] - 1, bound - tallies[receiver]) // 2
    margin = jnp.where((source_of == ranking[0]) | (receiver == ranking[0]) | (tallies[receiver] == 0), 0, jnp.maximum(margin, 0))
    shifted = jax.random.randint(jax.random.fold_in(own, 4), (count // 2,), 0, 1 << 20) % (margin + 1)
    tallies = tallies.at[source_of].add(-shifted).at[receiver].add(shifted)
    labels = jnp.searchsorted(jnp.cumsum(tallies), jnp.arange(rows * top), side="right").astype(jnp.int32)
    table = labels.reshape(top, rows).T
    table = table[jax.random.permutation(jax.random.fold_in(own, 1), rows)]
    turn = jax.random.randint(jax.random.fold_in(own, 2), (rows, 1), 0, top)
    return jnp.take_along_axis(table, (jnp.arange(top)[None, :] + turn) % top, axis=1)


def shares(amount, total, most, lean, full):
    loads = [(1 << 20) // math.isqrt(rank ** lean) + 1 for rank in range(1, amount + 1)]
    largest = most if full else min(most, max(-(-total // amount), total * loads[0] // sum(loads)))
    least = 1 if total - largest >= amount - 1 else 0
    holding, spare = [largest] + [least] * (amount - 1), total - largest - least * (amount - 1)
    while spare > 0:
        movable = [i for i in range(1, amount) if holding[i] < largest] or [i for i in range(1, amount) if holding[i] < most]
        whole, budget = sum([loads[i] for i in movable]), spare
        for i in movable:
            more = min(most - holding[i], max(1, budget * loads[i] // whole), spare)
            holding[i] = holding[i] + more
            spare = spare - more
    return np.array(holding)


def scatter_about(stream_key, shape, scale, most, cuts=(), kind=jnp.bfloat16):
    drawn = scale * jax.random.normal(stream_key, shape, jnp.float32)
    if cuts:
        drawn = drawn * levels(stream_key, shape, cuts, -0.22, 0.18)
    return jnp.clip(drawn, -most, most).astype(kind)


def setup_inputs(seed: int = 0, part: int = 0) -> dict:
    key_of = jax.random.split(jax.random.key(seed), 10)
    part_keys = jax.random.split(jax.random.fold_in(key_of[9], part), 10)
    tokens = scatter_about(part_keys[0], (TOKENS, D), 1.0, 6.0, ((0, 64),))
    routes_keys = jax.random.split(jax.random.fold_in(part_keys[1], 1), TOKENS // TOK_DEV)
    routes_turns = jax.random.permutation(jax.random.fold_in(part_keys[1], 3), TOKENS // TOK_DEV)
    routes = jax.vmap(lambda own, number: deal_out(jax.random.fold_in(part_keys[1], 2), own, number, TOK_DEV, EXPERTS, TOP, CAP, 2))(routes_keys, routes_turns).reshape((TOKENS, TOP))
    gates = jnp.clip(0.1 + 0.9 * jax.random.uniform(part_keys[2], (TOKENS, TOP), jnp.float32) ** levels(part_keys[2], (TOKENS, TOP), ((0, 64),), -0.2, 0.2), 0.1, 1.0)
    w_gate = scatter_about(key_of[3], (EXPERTS, D, FF), D ** -0.5, 0.15625, ((0, 64), (2, 2)))
    w_up = scatter_about(key_of[4], (EXPERTS, D, FF), D ** -0.5, 0.15625, ((0, 64), (2, 2)))
    w_down = scatter_about(key_of[5], (EXPERTS, FF, D), FF ** -0.5, 0.15625, ((0, 64), (1, 2)))
    shared_gate = scatter_about(key_of[6], (D, FS), D ** -0.5, 0.15625, ((1, 2),))
    shared_up = scatter_about(key_of[7], (D, FS), D ** -0.5, 0.15625, ((1, 2),))
    shared_down = scatter_about(key_of[8], (FS, D), FS ** -0.5, 0.15625, ((0, 2),))
    return {"tokens": tokens, "routes": routes, "gates": gates, "w_gate": w_gate, "w_up": w_up, "w_down": w_down, "shared_gate": shared_gate, "shared_up": shared_up, "shared_down": shared_down}


def reference(tokens, routes, gates, w_gate, w_up, w_down, shared_gate, shared_up, shared_down):
    blocked = routes.reshape(N_EXPERT, TOK_DEV * TOP)
    onehot = (blocked[:, :, None] == jnp.arange(EXPERTS, dtype=jnp.int32)[None, None, :]).astype(jnp.int32)
    order_in = jnp.sum(jnp.cumsum(onehot, axis=1) * onehot, axis=2) - 1
    source = jnp.arange(N_EXPERT, dtype=jnp.int32)[:, None]
    width_all = N_EXPERT * CAP
    slot_index = (blocked * width_all + source * CAP + order_in).reshape(-1).astype(jnp.int32)
    owner = jnp.repeat(jnp.arange(TOKENS, dtype=jnp.int32), TOP)
    token_of = jnp.full((EXPERTS * width_all,), TOKENS, jnp.int32).at[slot_index].set(owner)
    token_of = token_of.reshape(EXPERTS, width_all)
    padded = jnp.concatenate([tokens, jnp.zeros((1, D), tokens.dtype)], 0)

    def expert_rows(operands):
        index_rows, gate_mat, up_mat, down_mat = operands
        gathered = padded[index_rows]
        gate_val = jnp.dot(gathered, gate_mat, preferred_element_type=jnp.float32)
        up_val = jnp.dot(gathered, up_mat, preferred_element_type=jnp.float32)
        hidden = (jax.nn.silu(gate_val) * up_val).astype(jnp.bfloat16)
        return jnp.dot(hidden, down_mat, preferred_element_type=jnp.float32).astype(jnp.bfloat16)

    outputs = lax.map(expert_rows, (token_of, w_gate, w_up, w_down))
    picked = outputs.reshape(EXPERTS * width_all, D)[slot_index].reshape(TOKENS, TOP, D).astype(jnp.float32)
    routed = jnp.sum(gates[:, :, None] * picked, axis=1)
    shared_g = jnp.dot(tokens, shared_gate, preferred_element_type=jnp.float32)
    shared_u = jnp.dot(tokens, shared_up, preferred_element_type=jnp.float32)
    shared_hidden = (jax.nn.silu(shared_g) * shared_u).astype(jnp.bfloat16)
    shared_out = jnp.dot(shared_hidden, shared_down, preferred_element_type=jnp.float32)
    return (tokens.astype(jnp.float32) + routed + shared_out).astype(jnp.bfloat16)
```

```python
import functools

import jax
import jax.numpy as jnp
from jax import lax
from jax.experimental import pallas as pl
from jax.experimental.pallas import tpu as pltpu
from jax.sharding import PartitionSpec as P

COLUMNS = 4
META = 16
CHUNKS = 2
F32, BF16 = jnp.float32, jnp.bfloat16
VMEM = pl.BlockSpec(memory_space=pltpu.VMEM)
SMEM = pl.BlockSpec(memory_space=pltpu.SMEM)


def select_kernel(count, cap, half, where_ref, *refs):
    blocks = refs[: count * CHUNKS]
    outs = refs[count * CHUNKS : count * CHUNKS + COLUMNS]
    mix_ref = refs[-1]
    rows = sum(ref.shape[0] for ref in blocks[:CHUNKS])
    width = blocks[0].shape[1]
    before = lax.broadcasted_iota(jnp.int32, (rows, rows), 0)
    after = lax.broadcasted_iota(jnp.int32, (rows, rows), 1)
    upper = jnp.where(before <= after, 1.0, 0.0).astype(BF16)
    pick = lax.broadcasted_iota(jnp.int32, (META, width), 1) - half
    pick = jnp.where(pick == lax.broadcasted_iota(jnp.int32, (META, width), 0), 1.0, 0.0)
    pick = pick.astype(BF16)
    slot = lax.broadcasted_iota(jnp.int32, (cap, rows), 0).astype(F32)
    for i in range(count):
        block = jnp.concatenate([ref[...] for ref in blocks[i * CHUNKS : (i + 1) * CHUNKS]], 0)
        meta = lax.dot_general(pick, block, (((1,), (1,)), ((), ())), preferred_element_type=F32)
        named = meta[0:4].astype(jnp.int32)
        masks, highs, lows = [], [], []
        for j in range(COLUMNS):
            hit = jnp.where(named == where_ref[j], 1.0, 0.0)
            masks.append(jnp.sum(hit, axis=0, keepdims=True))
            highs.append(jnp.sum(hit * meta[4:8], axis=0, keepdims=True))
            lows.append(jnp.sum(hit * meta[8:12], axis=0, keepdims=True))
        mask = jnp.concatenate(masks, 0)
        rank = jnp.dot(mask.astype(BF16), upper, preferred_element_type=F32) - 1.0
        hots = []
        for j in range(COLUMNS):
            hots.append(jnp.where(slot == rank[j : j + 1], masks[j], 0.0))
        hot = jnp.concatenate(hots, 0)
        chosen = jnp.dot(hot.astype(BF16), block, preferred_element_type=F32).astype(BF16)
        for j in range(COLUMNS):
            outs[j][i] = chosen[j * cap : (j + 1) * cap, :half]
        high = jnp.concatenate([hots[j] * highs[j] for j in range(COLUMNS)], 0)
        low = jnp.concatenate([hots[j] * lows[j] for j in range(COLUMNS)], 0)
        mix_ref[i] = jnp.concatenate([high, low], 0).astype(BF16)


def select(blocks, where, cap, half):
    count = len(blocks)
    rows = sum(chunk.shape[0] for chunk in blocks[0])
    flops = count * 2 * COLUMNS * cap * rows * half
    return pl.pallas_call(
        functools.partial(select_kernel, count, cap, half),
        out_shape=[jax.ShapeDtypeStruct((count, cap, half), BF16)] * COLUMNS
        + [jax.ShapeDtypeStruct((count, 2 * COLUMNS * cap, rows), BF16)],
        in_specs=[SMEM] + [VMEM] * (count * CHUNKS),
        out_specs=[VMEM] * (COLUMNS + 1),
        cost_estimate=pl.CostEstimate(flops=4 * flops, bytes_accessed=count * rows * half * 4, transcendentals=0),
        name="select",
    )(where, *[chunk for block in blocks for chunk in block])


def ffn_kernel(own_row_ref, own_ref, other_ref, gate_ref, up_ref, keep_w_ref, send_w_ref, keep_ref, send_ref):
    half = own_ref.shape[1]
    mine = pl.ds(pl.multiple_of(own_row_ref[0], 8), half)
    theirs = pl.ds(pl.multiple_of(own_row_ref[1], 8), half)
    own, other = own_ref[...], other_ref[...]
    gate = jnp.dot(own, gate_ref[mine, :], preferred_element_type=F32)
    gate += jnp.dot(other, gate_ref[theirs, :], preferred_element_type=F32)
    up = jnp.dot(own, up_ref[mine, :], preferred_element_type=F32)
    up += jnp.dot(other, up_ref[theirs, :], preferred_element_type=F32)
    hidden = (jax.nn.silu(gate) * up).astype(BF16)
    send_ref[...] = jnp.dot(hidden, send_w_ref[...], preferred_element_type=F32)
    keep_ref[...] = jnp.dot(hidden, keep_w_ref[...], preferred_element_type=F32)


def ffn(starts, own, other, gate, up, keep_w, send_w):
    count, half = own.shape
    out = jax.ShapeDtypeStruct((count, half), F32)
    flops = 2 * count * (2 * gate.size + 2 * keep_w.size)
    return pl.pallas_call(
        ffn_kernel,
        out_shape=[out, out],
        in_specs=[SMEM] + [VMEM] * 6,
        out_specs=[VMEM] * 2,
        cost_estimate=pl.CostEstimate(flops=flops, bytes_accessed=8 * gate.size, transcendentals=count * half),
        name="ffn",
    )(starts, own, other, gate, up, keep_w, send_w)


def combine_kernel(mix_ref, *refs):
    parts, out_ref = refs[:-1], refs[-1]
    for i in range(mix_ref.shape[0]):
        values = jnp.concatenate([ref[i] for ref in parts] * 2, 0)
        out_ref[i] = lax.dot_general(mix_ref[i], values, (((0,), (0,)), ((), ())), preferred_element_type=F32)


def combine(mix, parts):
    count, cap, half = parts[0].shape
    rows = mix.shape[2]
    return pl.pallas_call(
        combine_kernel,
        out_shape=jax.ShapeDtypeStruct((count, rows, half), F32),
        in_specs=[VMEM] * (1 + len(parts)),
        out_specs=VMEM,
        cost_estimate=pl.CostEstimate(
            flops=2 * count * rows * mix.shape[1] * half, bytes_accessed=count * rows * half * 4, transcendentals=0
        ),
        name="combine",
    )(mix, *parts)


def local(tokens, routes, gates, w_gate, w_up, w_down, shared_gate, shared_up, shared_down):
    tok_count, top_count = routes.shape
    half = tokens.shape[1] // 2
    expert_count = lax.axis_size("expert")
    depth = expert_count // COLUMNS
    cap = max(2, (3 * tok_count * top_count + 2 * expert_count - 1) // (2 * expert_count))
    me, core = lax.axis_index("expert"), lax.axis_index("tensor")
    z_at, x_at = me // COLUMNS, me % COLUMNS
    where = jnp.stack([z_at * COLUMNS + (x_at + j) % COLUMNS for j in range(COLUMNS)]).astype(jnp.int32)
    starts = jnp.stack([core * half, (1 - core) * half]).astype(jnp.int32)

    def along_z(value, shift):
        pairs = [
            (z * COLUMNS + x, (z + shift) % depth * COLUMNS + x) for z in range(depth) for x in range(COLUMNS)
        ]
        return lax.ppermute(value, "expert", pairs)

    def along_x(value, shift):
        pairs = [
            (z * COLUMNS + x, z * COLUMNS + (x + shift) % COLUMNS) for z in range(depth) for x in range(COLUMNS)
        ]
        return lax.ppermute(value, "expert", pairs)

    def other_core(value):
        return lax.ppermute(value, "tensor", [(0, 1), (1, 0)])

    def halves(value, dim):
        mine = lax.dynamic_slice_in_dim(value, starts[0], half, dim)
        theirs = lax.dynamic_slice_in_dim(value, starts[1], half, dim)
        return mine, theirs

    own_cols, other_cols = halves(tokens, 1)
    high = lax.reduce_precision(gates, 8, 7)
    meta = [routes.astype(BF16), high.astype(BF16), (gates - high).astype(BF16)]
    spare = jnp.zeros((tok_count, META - 3 * top_count), BF16)
    payload = jnp.concatenate([own_cols] + meta + [spare], axis=1)
    piece = tok_count // CHUNKS
    mine = tuple(payload[c * piece : (c + 1) * piece] for c in range(CHUNKS))

    blocks = {0: mine}
    far = depth // 2
    for k in range(1, far + 1):
        for sign in (1, -1):
            if sign * k == -far:
                continue
            previous = blocks[sign * (k - 1)]
            blocks[sign * k] = tuple(along_z(chunk, sign) for chunk in previous)

    keep_w, send_w = halves(w_down[0], 1)
    shared_keep_w, shared_send_w = halves(shared_down, 1)
    shared_keep, shared_send = ffn(
        starts, own_cols, other_cols, shared_gate, shared_up, shared_keep_w, shared_send_w
    )
    shared = shared_keep + other_core(shared_send)

    order = [0] + [s * k for k in range(1, far) for s in (1, -1)] + [far]
    groups = group_blocks(order)
    partial = {}
    for group in groups:
        *picked, mix = select([blocks[d] for d in group], where, cap, half)
        came = [picked[0]] + [along_x(picked[j], j) for j in range(1, COLUMNS)]
        rows_own = jnp.concatenate(came, 0).reshape(-1, half)
        rows_other = other_core(rows_own)
        keep, send = ffn(starts, rows_own, rows_other, w_gate[0], w_up[0], keep_w, send_w)
        summed = (keep + other_core(send)).astype(BF16).reshape(COLUMNS, len(group), cap, half)
        back = [summed[0]] + [along_x(summed[j], -j) for j in range(1, COLUMNS)]
        parts = combine(mix, back)
        for i, d in enumerate(group):
            partial[d] = parts[i]

    def chunk_of(d, c):
        return partial[d][c * piece : (c + 1) * piece]

    totals = []
    for c in range(CHUNKS):
        arrived = []
        for sign in (1, -1):
            top = far if sign == 1 else far - 1
            moving = along_z(chunk_of(sign * top, c).astype(BF16), -sign)
            for k in range(top - 1, 0, -1):
                moving = (moving.astype(F32) + chunk_of(sign * k, c)).astype(BF16)
                moving = along_z(moving, -sign)
            arrived.append(moving.astype(F32))
        totals.append(chunk_of(0, c) + (arrived[0] + arrived[1]))
    routed = jnp.concatenate(totals, 0)
    return (own_cols.astype(F32) + (routed + shared)).astype(BF16)


def group_blocks(order):
    size = -(-len(order) // 4)
    first = len(order) - 3 * size + 1
    cuts = [order[:first + 0]]
    rest = order[first:]
    while rest:
        cuts.append(rest[:size])
        rest = rest[size:]
    return cuts


def solution(mesh):
    in_specs = (
        P(("groups", "expert"), None),
        P(("groups", "expert"), None),
        P(("groups", "expert"), None),
        P("expert", None, "tensor"),
        P("expert", None, "tensor"),
        P("expert", "tensor", None),
        P(None, "tensor"),
        P(None, "tensor"),
        P("tensor", None),
    )
    out_specs = P(("groups", "expert"), "tensor")
    return jax.shard_map(local, mesh=mesh, in_specs=in_specs, out_specs=out_specs, check_vma=False)
```

```python
import functools

import jax
import jax.numpy as jnp
from jax import lax
from jax.experimental import pallas as pl
from jax.experimental.pallas import tpu as pltpu
from jax.sharding import PartitionSpec as P

COLUMNS = 4
META = 16
CHUNKS = 2
GROUPS = ((1, 2, 3), (4, 5, 6), (7, 8))
F32, BF16 = jnp.float32, jnp.bfloat16
VMEM = pl.BlockSpec(memory_space=pltpu.VMEM)
SMEM = pl.BlockSpec(memory_space=pltpu.SMEM)


def select_kernel(count, cap, width, where_ref, *refs):
    blocks = refs[: count * CHUNKS]
    outs = refs[count * CHUNKS : count * CHUNKS + COLUMNS]
    mix_ref = refs[-1]
    rows = sum(ref.shape[0] for ref in blocks[:CHUNKS])
    base = width // 128 * 128
    tail = blocks[0].shape[1] - base
    before = lax.broadcasted_iota(jnp.int32, (rows, rows), 0)
    after = lax.broadcasted_iota(jnp.int32, (rows, rows), 1)
    upper = jnp.where(before <= after, 1.0, 0.0).astype(BF16)
    pick = lax.broadcasted_iota(jnp.int32, (META, tail), 1) - (width - base)
    pick = jnp.where(pick == lax.broadcasted_iota(jnp.int32, (META, tail), 0), 1.0, 0.0)
    pick = pick.astype(BF16)
    slot = lax.broadcasted_iota(jnp.int32, (cap, rows), 0).astype(F32)
    for i in range(count):
        block = jnp.concatenate([ref[...] for ref in blocks[i * CHUNKS : (i + 1) * CHUNKS]], 0)
        meta = lax.dot_general(
            pick, block[:, base:], (((1,), (1,)), ((), ())), preferred_element_type=F32
        )
        named = meta[0:4].astype(jnp.int32)
        masks, highs, lows = [], [], []
        for j in range(COLUMNS):
            hit = jnp.where(named == where_ref[j], 1.0, 0.0)
            masks.append(jnp.sum(hit, axis=0, keepdims=True))
            highs.append(jnp.sum(hit * meta[4:8], axis=0, keepdims=True))
            lows.append(jnp.sum(hit * meta[8:12], axis=0, keepdims=True))
        mask = jnp.concatenate(masks, 0)
        rank = jnp.dot(mask.astype(BF16), upper, preferred_element_type=F32) - 1.0
        hots = []
        for j in range(COLUMNS):
            hots.append(jnp.where(slot == rank[j : j + 1], masks[j], 0.0))
        hot = jnp.concatenate(hots, 0)
        chosen = jnp.dot(hot.astype(BF16), block, preferred_element_type=F32).astype(BF16)
        for j in range(COLUMNS):
            outs[j][i] = chosen[j * cap : (j + 1) * cap, :width]
        high = jnp.concatenate([hots[j] * highs[j] for j in range(COLUMNS)], 0)
        low = jnp.concatenate([hots[j] * lows[j] for j in range(COLUMNS)], 0)
        mix_ref[i] = jnp.concatenate([high, low], 0).astype(BF16)


def select(blocks, where, cap, width):
    count = len(blocks)
    rows = sum(chunk.shape[0] for chunk in blocks[0])
    flops = count * 2 * COLUMNS * cap * rows * width
    return pl.pallas_call(
        functools.partial(select_kernel, count, cap, width),
        out_shape=[jax.ShapeDtypeStruct((count, cap, width), BF16)] * COLUMNS
        + [jax.ShapeDtypeStruct((count, 2 * COLUMNS * cap, rows), BF16)],
        in_specs=[SMEM] + [VMEM] * (count * CHUNKS),
        out_specs=[VMEM] * (COLUMNS + 1),
        cost_estimate=pl.CostEstimate(
            flops=4 * flops, bytes_accessed=count * rows * width * 4, transcendentals=0
        ),
        name="select",
    )(where, *[chunk for block in blocks for chunk in block])


def ffn(inputs, gate, up, down):
    flops = sum(2 * 3 * value.size * gate.shape[1] for value in inputs)
    return pl.pallas_call(
        functools.partial(ffn_kernel, len(inputs)),
        out_shape=[jax.ShapeDtypeStruct(value.shape, F32) for value in inputs],
        in_specs=[VMEM] * (len(inputs) + 3),
        out_specs=[VMEM] * len(inputs),
        cost_estimate=pl.CostEstimate(flops=flops, bytes_accessed=6 * gate.size, transcendentals=0),
        name="ffn",
    )(*inputs, gate, up, down)


def ffn_kernel(count, *refs):
    inputs, outs = refs[:count], refs[count + 3 :]
    gate_ref, up_ref, down_ref = refs[count : count + 3]
    width = gate_ref.shape[0]
    rows = jnp.concatenate([ref[...].reshape(-1, width) for ref in inputs], 0)
    gate = jnp.dot(rows, gate_ref[...], preferred_element_type=F32)
    up = jnp.dot(rows, up_ref[...], preferred_element_type=F32)
    hidden = (jax.nn.silu(gate) * up).astype(BF16)
    result = jnp.dot(hidden, down_ref[...], preferred_element_type=F32)
    at = 0
    for ref, out in zip(inputs, outs):
        size = rows.shape[0] // count
        out[...] = result[at : at + size].reshape(out.shape)
        at += size


def join_kernel(keep_ref, came_ref, *outs):
    count = outs[0].shape[0]
    for j, out in enumerate(outs):
        part = slice(j * count, (j + 1) * count)
        out[...] = (keep_ref[part] + came_ref[part]).astype(BF16)


def join(keep, came):
    total, cap, width = keep.shape
    out = jax.ShapeDtypeStruct((total // COLUMNS, cap, width), BF16)
    return pl.pallas_call(
        join_kernel,
        out_shape=[out] * COLUMNS,
        in_specs=[VMEM] * 2,
        out_specs=[VMEM] * COLUMNS,
        cost_estimate=pl.CostEstimate(flops=20 * keep.size, bytes_accessed=10 * keep.size, transcendentals=0),
        name="join",
    )(keep, came)


def combine_kernel(mix_ref, *refs):
    parts, out_ref = refs[:COLUMNS], refs[-1]
    values = jnp.concatenate([ref[0] for ref in parts] * 2, 0)
    result = lax.dot_general(mix_ref[0], values, (((0,), (0,)), ((), ())), preferred_element_type=F32)
    if len(refs) > COLUMNS + 1:
        result += refs[COLUMNS][...].astype(F32)
    out_ref[...] = result.astype(BF16)


def combine(mix, parts, i, c, came):
    _, cap, width = parts[0].shape
    rows = mix.shape[2] // CHUNKS
    whole = pl.BlockSpec((rows, width), lambda g: (0, 0))
    extra = [] if came is None else [came]
    return pl.pallas_call(
        combine_kernel,
        grid=(1,),
        out_shape=jax.ShapeDtypeStruct((rows, width), BF16),
        in_specs=[pl.BlockSpec((1, mix.shape[1], rows), lambda g: (i, 0, c))]
        + [pl.BlockSpec((1, cap, width), lambda g: (i, 0, 0))] * COLUMNS
        + [whole] * len(extra),
        out_specs=whole,
        cost_estimate=pl.CostEstimate(
            flops=2 * rows * mix.shape[1] * width, bytes_accessed=4 * rows * width, transcendentals=0
        ),
        name="combine",
    )(mix, *parts, *extra)


def after(value, *things):
    return lax.optimization_barrier((value, *things))[0]


def local(tokens, routes, gates, w_gate, w_up, w_down, shared_gate, shared_up, shared_down):
    tok_count, top_count = routes.shape
    width = tokens.shape[1]
    half = width // 2
    expert_count = lax.axis_size("expert")
    depth = expert_count // COLUMNS
    steps = depth // 2
    cap = max(2, (3 * tok_count * top_count + 2 * expert_count - 1) // (2 * expert_count))
    me, core = lax.axis_index("expert"), lax.axis_index("tensor")
    turn = (me & (COLUMNS - 1)) + jnp.arange(COLUMNS, dtype=jnp.int32)
    where = (me & ~(COLUMNS - 1)) + (turn & (COLUMNS - 1))

    def ring(value, step, back):
        pairs = []
        for z in range(depth):
            for x in range(COLUMNS):
                for c in range(2):
                    shift = (1 if c == 0 else -1) * (-1 if back else 1)
                    if step == 1 and c == 1:
                        shift = 0
                    to = (z + shift) % depth
                    pairs.append(((z * COLUMNS + x) * 2 + c, (to * COLUMNS + x) * 2 + c))
        return lax.ppermute(value, ("expert", "tensor"), pairs)

    def along_x(value, shift):
        pairs = [
            (z * COLUMNS + x, z * COLUMNS + (x + shift) % COLUMNS) for z in range(depth) for x in range(COLUMNS)
        ]
        return lax.ppermute(value, "expert", pairs)

    def other_core(value):
        return lax.ppermute(value, "tensor", [(0, 1), (1, 0)])

    def split(value):
        low, high = value[:, :half], value[:, half:]
        return jnp.where(core == 0, low, high), jnp.where(core == 0, high, low)

    high = lax.reduce_precision(gates, 8, 7)
    meta = [routes.astype(BF16), high.astype(BF16), (gates - high).astype(BF16)]
    spare = jnp.zeros((tok_count, META - 3 * top_count), BF16)
    payload = jnp.concatenate([tokens] + meta + [spare], axis=1)
    piece = tok_count // CHUNKS
    held = [payload[c * piece : (c + 1) * piece] for c in range(CHUNKS)]

    state = {}

    def work_select(g):
        *picked, mix = select([state["block", k] for k in GROUPS[g]], where, cap, width)
        state["mix", g] = mix
        state["picked", g] = picked
        return mix

    def work_send(g):
        picked = state["picked", g]
        state["came", g] = [picked[0]] + [along_x(picked[j], j) for j in range(1, COLUMNS)]

    def work_swap(g):
        own = jnp.concatenate(state["came", g], 0)
        state["own", g] = own
        state["other", g] = other_core(own)
        return own

    def work_ffn(g):
        keep, send = ffn([state["own", g], state["other", g]], w_gate[0], w_up[0], w_down[0])
        state["keep", g] = keep
        state["partial", g] = other_core(send)
        return keep

    def work_back(g):
        summed = join(state["keep", g], state["partial", g])
        state["back", g] = [summed[0]] + [along_x(summed[j], -j) for j in range(1, COLUMNS)]
        return summed[0]

    def work_shared():
        (mine,) = ffn([tokens], shared_gate, shared_up, shared_down)
        keep, send = split(mine)
        state["shared"] = (keep, send)
        return keep

    between = {1: [work_shared]}
    for g, group in enumerate(GROUPS[:-1]):
        k = group[-1] + 1
        stages = [work_select, work_swap, work_ffn, work_back]
        for s, stage in enumerate(stages):
            between.setdefault(k + s, []).append(functools.partial(stage, g))

    done = set()
    for k in range(1, steps + 1):
        arriving = [ring(chunk, k, False) for chunk in held]
        state["block", k] = arriving
        things = []
        for stage in between.get(k, []):
            things.append(stage())
            key = (getattr(stage, "func", stage), getattr(stage, "args", ()))
            done.add(key)
            if key[0] is work_select:
                work_send(key[1][0])
        held = list(arriving)
        if things and k < steps:
            held[0] = after(held[0], *things)

    last = len(GROUPS) - 1
    work_select(last)
    work_send(last)
    for g in range(last + 1):
        for stage in (work_swap, work_ffn, work_back):
            if (stage, (g,)) not in done:
                stage(g)

    shared_keep, shared_send = state["shared"]
    own_cols, _ = split(tokens)
    base = own_cols.astype(F32) + (shared_keep + other_core(shared_send))

    moving = [None] * CHUNKS
    for k in range(steps, 0, -1):
        g = next(n for n, group in enumerate(GROUPS) if k in group)
        i = GROUPS[g].index(k)
        for c in range(CHUNKS):
            total = combine(state["mix", g], state["back", g], i, c, moving[c])
            moving[c] = ring(total, k, True)
    kept, sent = split(jnp.concatenate(moving, 0))
    routed = kept.astype(F32) + other_core(sent).astype(F32)
    return (base + routed).astype(BF16)


def solution(mesh):
    in_specs = (
        P(("groups", "expert"), None),
        P(("groups", "expert"), None),
        P(("groups", "expert"), None),
        P("expert", None, "tensor"),
        P("expert", None, "tensor"),
        P("expert", "tensor", None),
        P(None, "tensor"),
        P(None, "tensor"),
        P("tensor", None),
    )
    out_specs = P(("groups", "expert"), "tensor")
    return jax.shard_map(local, mesh=mesh, in_specs=in_specs, out_specs=out_specs, check_vma=False)
```

```python
import functools

import jax
import jax.numpy as jnp
from jax import lax
from jax.experimental import pallas as pl
from jax.experimental.pallas import tpu as pltpu
from jax.sharding import PartitionSpec as P

COLUMNS = 4
META = 16
CHUNKS = 2
GROUPS = ((1, 2, 3, 4, 5), (6, 7, 8))
F32, BF16 = jnp.float32, jnp.bfloat16
VMEM = pl.BlockSpec(memory_space=pltpu.VMEM)
SMEM = pl.BlockSpec(memory_space=pltpu.SMEM)


def select_kernel(count, cap, width, first_ref, *refs):
    blocks = refs[: count * CHUNKS]
    rows_ref, mixes = refs[count * CHUNKS], refs[count * CHUNKS + 1 :]
    rows = sum(ref.shape[0] for ref in blocks[:CHUNKS])
    piece = rows // CHUNKS
    base = width // 128 * 128
    tail = blocks[0].shape[1] - base
    before = lax.broadcasted_iota(jnp.int32, (rows, rows), 0)
    after = lax.broadcasted_iota(jnp.int32, (rows, rows), 1)
    upper = jnp.where(before <= after, 1.0, 0.0).astype(BF16)
    pick = lax.broadcasted_iota(jnp.int32, (META, tail), 1) - (width - base)
    pick = jnp.where(pick == lax.broadcasted_iota(jnp.int32, (META, tail), 0), 1.0, 0.0)
    pick = pick.astype(BF16)
    slot = lax.broadcasted_iota(jnp.int32, (cap, rows), 0).astype(F32)
    for i in range(count):
        block = jnp.concatenate([ref[...] for ref in blocks[i * CHUNKS : (i + 1) * CHUNKS]], 0)
        meta = lax.dot_general(
            pick, block[:, base:], (((1,), (1,)), ((), ())), preferred_element_type=F32
        )
        named = meta[0:4].astype(jnp.int32)
        masks, highs, lows = [], [], []
        for j in range(COLUMNS):
            hit = jnp.where(named == first_ref[0] + j, 1.0, 0.0)
            masks.append(jnp.sum(hit, axis=0, keepdims=True))
            highs.append(jnp.sum(hit * meta[4:8], axis=0, keepdims=True))
            lows.append(jnp.sum(hit * meta[8:12], axis=0, keepdims=True))
        mask = jnp.concatenate(masks, 0)
        rank = jnp.dot(mask.astype(BF16), upper, preferred_element_type=F32) - 1.0
        hots = []
        for j in range(COLUMNS):
            hots.append(jnp.where(slot == rank[j : j + 1], masks[j], 0.0))
        hot = jnp.concatenate(hots, 0)
        chosen = jnp.dot(hot.astype(BF16), block, preferred_element_type=F32).astype(BF16)
        for j in range(COLUMNS):
            rows_ref[j, i] = chosen[j * cap : (j + 1) * cap, :width]
        high = jnp.concatenate([hots[j] * highs[j] for j in range(COLUMNS)], 0)
        low = jnp.concatenate([hots[j] * lows[j] for j in range(COLUMNS)], 0)
        mix = jnp.concatenate([high, low], 0).astype(BF16)
        for c in range(CHUNKS):
            mixes[i * CHUNKS + c][...] = mix[:, c * piece : (c + 1) * piece]


def select(blocks, first, cap, width):
    count = len(blocks)
    rows = sum(chunk.shape[0] for chunk in blocks[0])
    flops = count * 2 * COLUMNS * cap * rows * width
    picked, *mixes = pl.pallas_call(
        functools.partial(select_kernel, count, cap, width),
        out_shape=[jax.ShapeDtypeStruct((COLUMNS, count, cap, width), BF16)]
        + [jax.ShapeDtypeStruct((2 * COLUMNS * cap, rows // CHUNKS), BF16)] * (count * CHUNKS),
        in_specs=[SMEM] + [VMEM] * (count * CHUNKS),
        out_specs=[VMEM] * (1 + count * CHUNKS),
        cost_estimate=pl.CostEstimate(
            flops=4 * flops, bytes_accessed=count * rows * width * 4, transcendentals=0
        ),
        name="select",
    )(first, *[chunk for block in blocks for chunk in block])
    return picked, [mixes[i * CHUNKS : (i + 1) * CHUNKS] for i in range(count)]


def ffn(inputs, gate, up, down):
    flops = sum(2 * 3 * value.size * gate.shape[1] for value in inputs)
    return pl.pallas_call(
        functools.partial(ffn_kernel, len(inputs)),
        out_shape=[jax.ShapeDtypeStruct(value.shape, F32) for value in inputs],
        in_specs=[VMEM] * (len(inputs) + 3),
        out_specs=[VMEM] * len(inputs),
        cost_estimate=pl.CostEstimate(flops=flops, bytes_accessed=6 * gate.size, transcendentals=0),
        name="ffn",
    )(*inputs, gate, up, down)


def ffn_kernel(count, *refs):
    inputs, outs = refs[:count], refs[count + 3 :]
    gate_ref, up_ref, down_ref = refs[count : count + 3]
    width = gate_ref.shape[0]
    rows = jnp.concatenate([ref[...].reshape(-1, width) for ref in inputs], 0)
    gate = jnp.dot(rows, gate_ref[...], preferred_element_type=F32)
    up = jnp.dot(rows, up_ref[...], preferred_element_type=F32)
    hidden = (jax.nn.silu(gate) * up).astype(BF16)
    result = jnp.dot(hidden, down_ref[...], preferred_element_type=F32)
    at = 0
    for ref, out in zip(inputs, outs):
        size = rows.shape[0] // count
        out[...] = result[at : at + size].reshape(out.shape)
        at += size


def join_kernel(keep_ref, came_ref, out_ref):
    out_ref[...] = (keep_ref[...] + came_ref[...]).astype(BF16)


def join(keep, came):
    return pl.pallas_call(
        join_kernel,
        out_shape=jax.ShapeDtypeStruct(keep.shape, BF16),
        in_specs=[VMEM] * 2,
        out_specs=VMEM,
        cost_estimate=pl.CostEstimate(flops=20 * keep.size, bytes_accessed=10 * keep.size, transcendentals=0),
        name="join",
    )(keep, came)


def spread_kernel(back_ref, *outs):
    cap = back_ref.shape[2]
    for i, out in enumerate(outs):
        for n in range(2 * COLUMNS):
            out[n * cap : (n + 1) * cap] = back_ref[n % COLUMNS, i]


def spread(back):
    _, count, cap, width = back.shape
    return pl.pallas_call(
        spread_kernel,
        out_shape=[jax.ShapeDtypeStruct((2 * COLUMNS * cap, width), BF16)] * count,
        in_specs=[VMEM],
        out_specs=[VMEM] * count,
        cost_estimate=pl.CostEstimate(flops=20 * back.size, bytes_accessed=6 * back.size, transcendentals=0),
        name="spread",
    )(back)


def local(tokens, routes, gates, w_gate, w_up, w_down, shared_gate, shared_up, shared_down):
    tok_count, top_count = routes.shape
    width = tokens.shape[1]
    half = width // 2
    expert_count = lax.axis_size("expert")
    depth = expert_count // COLUMNS
    steps = depth // 2
    cap = max(2, (3 * tok_count * top_count + 2 * expert_count - 1) // (2 * expert_count))
    me, core = lax.axis_index("expert"), lax.axis_index("tensor")
    first = (me & ~(COLUMNS - 1)).reshape(1).astype(jnp.int32)

    def ring(value, step, back):
        pairs = []
        for z in range(depth):
            for x in range(COLUMNS):
                for c in range(2):
                    shift = (1 if c == 0 else -1) * (-1 if back else 1)
                    if step == 1 and c == 1:
                        shift = 0
                    to = (z + shift) % depth
                    pairs.append(((z * COLUMNS + x) * 2 + c, (to * COLUMNS + x) * 2 + c))
        return lax.ppermute(value, ("expert", "tensor"), pairs)

    def along_x(value):
        rows = [[z * COLUMNS + x for x in range(COLUMNS)] for z in range(depth)]
        return lax.all_to_all(value, "expert", 0, 0, axis_index_groups=rows, tiled=True)

    def other_core(value):
        return lax.ppermute(value, "tensor", [(0, 1), (1, 0)])

    def split(value):
        low, high = value[:, :half], value[:, half:]
        return jnp.where(core == 0, low, high), jnp.where(core == 0, high, low)

    high = lax.reduce_precision(gates, 8, 7)
    meta = [routes.astype(BF16), high.astype(BF16), (gates - high).astype(BF16)]
    spare = jnp.zeros((tok_count, META - 3 * top_count), BF16)
    payload = jnp.concatenate([tokens] + meta + [spare], axis=1)
    piece = tok_count // CHUNKS
    held = [payload[c * piece : (c + 1) * piece] for c in range(CHUNKS)]

    blocks = {}
    for k in range(1, steps + 1):
        for c in range(CHUNKS):
            held[c] = ring(held[c], k, False)
        blocks[k] = list(held)

    (shared_part,) = ffn([tokens], shared_gate, shared_up, shared_down)
    shared_keep, shared_send = split(shared_part)
    own_cols, _ = split(tokens)
    shared_came = other_core(shared_send)
    base = own_cols.astype(F32) + (shared_keep + shared_came)

    mixes, values = {}, {}
    for group in GROUPS:
        picked, mix = select([blocks[k] for k in group], first, cap, width)
        own = along_x(picked)
        other = other_core(own)
        keep, send = ffn([own, other], w_gate[0], w_up[0], w_down[0])
        came = other_core(send)
        summed = join(keep, came)
        back = along_x(summed)
        rows = spread(back)
        for i, k in enumerate(group):
            mixes[k], values[k] = mix[i], rows[i]

    moving = [None] * CHUNKS
    for k in range(steps, 0, -1):
        for c in range(CHUNKS):
            total = lax.dot_general(
                mixes[k][c], values[k], (((0,), (0,)), ((), ())), preferred_element_type=F32
            )
            if moving[c] is not None:
                total += moving[c].astype(F32)
            total = total.astype(BF16)
            moving[c] = ring(total, k, True)
    kept, sent = [], []
    for c in range(CHUNKS):
        keep, send = split(moving[c])
        kept.append(keep)
        sent.append(other_core(send))
    routed = jnp.concatenate(kept, 0).astype(F32) + jnp.concatenate(sent, 0).astype(F32)
    return (base + routed).astype(BF16)


def solution(mesh):
    in_specs = (
        P(("groups", "expert"), None),
        P(("groups", "expert"), None),
        P(("groups", "expert"), None),
        P("expert", None, "tensor"),
        P("expert", None, "tensor"),
        P("expert", "tensor", None),
        P(None, "tensor"),
        P(None, "tensor"),
        P("tensor", None),
    )
    out_specs = P(("groups", "expert"), "tensor")

    return jax.shard_map(local, mesh=mesh, in_specs=in_specs, out_specs=out_specs, check_vma=False)
```

```python
import functools

import jax
import jax.numpy as jnp
from jax import lax
from jax.experimental import pallas as pl
from jax.experimental.pallas import tpu as pltpu
from jax.sharding import PartitionSpec as P

COLUMNS = 4
META = 16
CHUNKS = 2
GROUPS = ((1, 2, 3), (4, 5, 6), (7, 8))
F32, BF16 = jnp.float32, jnp.bfloat16
VMEM = pl.BlockSpec(memory_space=pltpu.VMEM)
SMEM = pl.BlockSpec(memory_space=pltpu.SMEM)


def select_kernel(count, cap, width, where_ref, *refs):
    blocks = refs[: count * CHUNKS]
    outs = refs[count * CHUNKS : count * CHUNKS + COLUMNS]
    mixes = refs[count * CHUNKS + COLUMNS :]
    rows = sum(ref.shape[0] for ref in blocks[:CHUNKS])
    piece = rows // CHUNKS
    base = width // 128 * 128
    tail = blocks[0].shape[1] - base
    before = lax.broadcasted_iota(jnp.int32, (rows, rows), 0)
    after = lax.broadcasted_iota(jnp.int32, (rows, rows), 1)
    upper = jnp.where(before <= after, 1.0, 0.0).astype(BF16)
    pick = lax.broadcasted_iota(jnp.int32, (META, tail), 1) - (width - base)
    pick = jnp.where(pick == lax.broadcasted_iota(jnp.int32, (META, tail), 0), 1.0, 0.0)
    pick = pick.astype(BF16)
    slot = lax.broadcasted_iota(jnp.int32, (cap, rows), 0).astype(F32)
    for i in range(count):
        block = jnp.concatenate([ref[...] for ref in blocks[i * CHUNKS : (i + 1) * CHUNKS]], 0)
        meta = lax.dot_general(
            pick, block[:, base:], (((1,), (1,)), ((), ())), preferred_element_type=F32
        )
        named = meta[0:4].astype(jnp.int32)
        masks, highs, lows = [], [], []
        for j in range(COLUMNS):
            hit = jnp.where(named == where_ref[j], 1.0, 0.0)
            masks.append(jnp.sum(hit, axis=0, keepdims=True))
            highs.append(jnp.sum(hit * meta[4:8], axis=0, keepdims=True))
            lows.append(jnp.sum(hit * meta[8:12], axis=0, keepdims=True))
        mask = jnp.concatenate(masks, 0)
        rank = jnp.dot(mask.astype(BF16), upper, preferred_element_type=F32) - 1.0
        hots = []
        for j in range(COLUMNS):
            hots.append(jnp.where(slot == rank[j : j + 1], masks[j], 0.0))
        hot = jnp.concatenate(hots, 0)
        chosen = jnp.dot(hot.astype(BF16), block, preferred_element_type=F32).astype(BF16)
        for j in range(COLUMNS):
            outs[j][i] = chosen[j * cap : (j + 1) * cap, :width]
        high = jnp.concatenate([hots[j] * highs[j] for j in range(COLUMNS)], 0)
        low = jnp.concatenate([hots[j] * lows[j] for j in range(COLUMNS)], 0)
        mix = jnp.concatenate([high, low], 0).astype(BF16)
        for c in range(CHUNKS):
            mixes[i * CHUNKS + c][...] = mix[:, c * piece : (c + 1) * piece]


def select(blocks, where, cap, width):
    count = len(blocks)
    rows = sum(chunk.shape[0] for chunk in blocks[0])
    flops = count * 2 * COLUMNS * cap * rows * width
    outs = pl.pallas_call(
        functools.partial(select_kernel, count, cap, width),
        out_shape=[jax.ShapeDtypeStruct((count, cap, width), BF16)] * COLUMNS
        + [jax.ShapeDtypeStruct((2 * COLUMNS * cap, rows // CHUNKS), BF16)] * (count * CHUNKS),
        in_specs=[SMEM] + [VMEM] * (count * CHUNKS),
        out_specs=[VMEM] * (COLUMNS + count * CHUNKS),
        cost_estimate=pl.CostEstimate(
            flops=4 * flops, bytes_accessed=count * rows * width * 4, transcendentals=0
        ),
        name="select",
    )(where, *[chunk for block in blocks for chunk in block])
    picked, mixes = outs[:COLUMNS], outs[COLUMNS:]
    return picked, [mixes[i * CHUNKS : (i + 1) * CHUNKS] for i in range(count)]


def ffn(inputs, outs, gate, up, down):
    flops = sum(2 * 3 * value.size * gate.shape[1] for value in inputs)
    return pl.pallas_call(
        functools.partial(ffn_kernel, len(inputs)),
        out_shape=[jax.ShapeDtypeStruct(shape, F32) for shape in outs],
        in_specs=[VMEM] * (len(inputs) + 3),
        out_specs=[VMEM] * len(outs),
        cost_estimate=pl.CostEstimate(flops=flops, bytes_accessed=6 * gate.size, transcendentals=0),
        name="ffn",
    )(*inputs, gate, up, down)


def ffn_kernel(count, *refs):
    inputs, outs = refs[:count], refs[count + 3 :]
    gate_ref, up_ref, down_ref = refs[count : count + 3]
    width = gate_ref.shape[0]
    rows = jnp.concatenate([ref[...].reshape(-1, width) for ref in inputs], 0)
    gate = jnp.dot(rows, gate_ref[...], preferred_element_type=F32)
    up = jnp.dot(rows, up_ref[...], preferred_element_type=F32)
    hidden = (jax.nn.silu(gate) * up).astype(BF16)
    result = jnp.dot(hidden, down_ref[...], preferred_element_type=F32)
    size = rows.shape[0] // len(outs)
    for n, out in enumerate(outs):
        out[...] = result[n * size : (n + 1) * size].reshape(out.shape)


def join_kernel(keep_ref, came_ref, *outs):
    count = outs[0].shape[0]
    for j, out in enumerate(outs):
        part = slice(j * count, (j + 1) * count)
        out[...] = (keep_ref[part] + came_ref[part]).astype(BF16)


def join(keep, came):
    total, cap, width = keep.shape
    return pl.pallas_call(
        join_kernel,
        out_shape=[jax.ShapeDtypeStruct((total // COLUMNS, cap, width), BF16)] * COLUMNS,
        in_specs=[VMEM] * 2,
        out_specs=[VMEM] * COLUMNS,
        cost_estimate=pl.CostEstimate(flops=20 * keep.size, bytes_accessed=10 * keep.size, transcendentals=0),
        name="join",
    )(keep, came)


def spread_kernel(*refs):
    parts, outs = refs[:COLUMNS], refs[COLUMNS:]
    cap = parts[0].shape[1]
    for i, out in enumerate(outs):
        for n in range(2 * COLUMNS):
            out[n * cap : (n + 1) * cap] = parts[n % COLUMNS][i]


def spread(parts):
    count, cap, width = parts[0].shape
    size = COLUMNS * parts[0].size
    return pl.pallas_call(
        spread_kernel,
        out_shape=[jax.ShapeDtypeStruct((2 * COLUMNS * cap, width), BF16)] * count,
        in_specs=[VMEM] * COLUMNS,
        out_specs=[VMEM] * count,
        cost_estimate=pl.CostEstimate(flops=20 * size, bytes_accessed=6 * size, transcendentals=0),
        name="spread",
    )(*parts)


def local(tokens, routes, gates, w_gate, w_up, w_down, shared_gate, shared_up, shared_down):
    tok_count, top_count = routes.shape
    width = tokens.shape[1]
    half = width // 2
    expert_count = lax.axis_size("expert")
    depth = expert_count // COLUMNS
    steps = depth // 2
    cap = max(2, (3 * tok_count * top_count + 2 * expert_count - 1) // (2 * expert_count))
    me, core = lax.axis_index("expert"), lax.axis_index("tensor")
    turn = (me & (COLUMNS - 1)) + jnp.arange(COLUMNS, dtype=jnp.int32)
    where = (me & ~(COLUMNS - 1)) + (turn & (COLUMNS - 1))

    def ring(value, step, back):
        pairs = []
        for z in range(depth):
            for x in range(COLUMNS):
                for c in range(2):
                    shift = (1 if c == 0 else -1) * (-1 if back else 1)
                    if step == 1 and c == 1:
                        shift = 0
                    to = (z + shift) % depth
                    pairs.append(((z * COLUMNS + x) * 2 + c, (to * COLUMNS + x) * 2 + c))
        return lax.ppermute(value, ("expert", "tensor"), pairs)

    def along_x(value, shift):
        pairs = [
            (z * COLUMNS + x, z * COLUMNS + (x + shift) % COLUMNS) for z in range(depth) for x in range(COLUMNS)
        ]
        return lax.ppermute(value, "expert", pairs)

    def other_core(value):
        return lax.ppermute(value, "tensor", [(0, 1), (1, 0)])

    def split(value):
        low, high = value[:, :half], value[:, half:]
        return jnp.where(core == 0, low, high), jnp.where(core == 0, high, low)

    high = lax.reduce_precision(gates, 8, 7)
    meta = [routes.astype(BF16), high.astype(BF16), (gates - high).astype(BF16)]
    spare = jnp.zeros((tok_count, META - 3 * top_count), BF16)
    payload = jnp.concatenate([tokens] + meta + [spare], axis=1)
    piece = tok_count // CHUNKS
    held = [payload[c * piece : (c + 1) * piece] for c in range(CHUNKS)]

    blocks = {}
    for k in range(1, steps + 1):
        for c in range(CHUNKS):
            held[c] = ring(held[c], k, False)
        blocks[k] = list(held)

    (shared_part,) = ffn([tokens], [tokens.shape], shared_gate, shared_up, shared_down)
    shared_keep, shared_send = split(shared_part)
    own_cols, _ = split(tokens)
    shared_came = other_core(shared_send)
    base = lax.optimization_barrier(own_cols.astype(F32) + (shared_keep + shared_came))

    mixes, values = {}, {}
    for group in GROUPS:
        picked, mix = select([blocks[k] for k in group], where, cap, width)
        own = [picked[0]]
        for j in range(1, COLUMNS):
            own.append(along_x(picked[j], j))
        other = []
        for j in range(COLUMNS):
            other.append(other_core(own[j]))
        shape = (COLUMNS * len(group), cap, width)
        keep, send = ffn(own + other, [shape, shape], w_gate[0], w_up[0], w_down[0])
        came = other_core(send)
        summed = join(keep, came)
        back = [summed[0]]
        for j in range(1, COLUMNS):
            back.append(along_x(summed[j], -j))
        rows = spread(back)
        for i, k in enumerate(group):
            mixes[k], values[k] = mix[i], rows[i]

    moving = [None] * CHUNKS
    for k in range(steps, 0, -1):
        for c in range(CHUNKS):
            total = lax.dot_general(
                mixes[k][c], values[k], (((0,), (0,)), ((), ())), preferred_element_type=F32
            )
            if moving[c] is not None:
                total += moving[c].astype(F32)
            total = total.astype(BF16)
            moving[c] = ring(total, k, True)
    kept, sent = [], []
    for c in range(CHUNKS):
        keep, send = split(moving[c])
        kept.append(keep)
        sent.append(other_core(send))
    routed = jnp.concatenate(kept, 0).astype(F32) + jnp.concatenate(sent, 0).astype(F32)
    return (base + routed).astype(BF16)


def solution(mesh):
    in_specs = (
        P(("groups", "expert"), None),
        P(("groups", "expert"), None),
        P(("groups", "expert"), None),
        P("expert", None, "tensor"),
        P("expert", None, "tensor"),
        P("expert", "tensor", None),
        P(None, "tensor"),
        P(None, "tensor"),
        P("tensor", None),
    )
    out_specs = P(("groups", "expert"), "tensor")

    return jax.shard_map(local, mesh=mesh, in_specs=in_specs, out_specs=out_specs, check_vma=False)
```

```python
import functools

import jax
import jax.numpy as jnp
from jax import lax
from jax.experimental import pallas as pl
from jax.experimental.pallas import tpu as pltpu
from jax.sharding import PartitionSpec as P

COLUMNS = 4
META = 16
CHUNKS = 2
GROUPS = ((1, 2, 3), (4, 5, 6), (7, 8))
F32, BF16 = jnp.float32, jnp.bfloat16
VMEM = pl.BlockSpec(memory_space=pltpu.VMEM)
SMEM = pl.BlockSpec(memory_space=pltpu.SMEM)


def close(value):
    return pltpu.with_memory_space_constraint(value, pltpu.VMEM)


def select_kernel(count, cap, width, where_ref, *refs):
    blocks = refs[: count * CHUNKS]
    outs = refs[count * CHUNKS : count * CHUNKS + COLUMNS]
    mixes = refs[count * CHUNKS + COLUMNS :]
    rows = sum(ref.shape[0] for ref in blocks[:CHUNKS])
    piece = rows // CHUNKS
    base = width // 128 * 128
    tail = blocks[0].shape[1] - base
    before = lax.broadcasted_iota(jnp.int32, (rows, rows), 0)
    after = lax.broadcasted_iota(jnp.int32, (rows, rows), 1)
    upper = jnp.where(before <= after, 1.0, 0.0).astype(BF16)
    pick = lax.broadcasted_iota(jnp.int32, (META, tail), 1) - (width - base)
    pick = jnp.where(pick == lax.broadcasted_iota(jnp.int32, (META, tail), 0), 1.0, 0.0)
    pick = pick.astype(BF16)
    slot = lax.broadcasted_iota(jnp.int32, (cap, rows), 0).astype(F32)
    for i in range(count):
        block = jnp.concatenate([ref[...] for ref in blocks[i * CHUNKS : (i + 1) * CHUNKS]], 0)
        meta = lax.dot_general(
            pick, block[:, base:], (((1,), (1,)), ((), ())), preferred_element_type=F32
        )
        named = meta[0:4].astype(jnp.int32)
        masks, highs, lows = [], [], []
        for j in range(COLUMNS):
            hit = jnp.where(named == where_ref[j], 1.0, 0.0)
            masks.append(jnp.sum(hit, axis=0, keepdims=True))
            highs.append(jnp.sum(hit * meta[4:8], axis=0, keepdims=True))
            lows.append(jnp.sum(hit * meta[8:12], axis=0, keepdims=True))
        mask = jnp.concatenate(masks, 0)
        rank = jnp.dot(mask.astype(BF16), upper, preferred_element_type=F32) - 1.0
        hots = []
        for j in range(COLUMNS):
            hots.append(jnp.where(slot == rank[j : j + 1], masks[j], 0.0))
        hot = jnp.concatenate(hots, 0)
        chosen = jnp.dot(hot.astype(BF16), block, preferred_element_type=F32).astype(BF16)
        for j in range(COLUMNS):
            outs[j][i] = chosen[j * cap : (j + 1) * cap, :width]
        high = jnp.concatenate([hots[j] * highs[j] for j in range(COLUMNS)], 0)
        low = jnp.concatenate([hots[j] * lows[j] for j in range(COLUMNS)], 0)
        mix = jnp.concatenate([high, low], 0).astype(BF16)
        for c in range(CHUNKS):
            mixes[i * CHUNKS + c][...] = mix[:, c * piece : (c + 1) * piece]


def select(blocks, where, cap, width):
    count = len(blocks)
    rows = sum(chunk.shape[0] for chunk in blocks[0])
    flops = count * 2 * COLUMNS * cap * rows * width
    outs = pl.pallas_call(
        functools.partial(select_kernel, count, cap, width),
        out_shape=[jax.ShapeDtypeStruct((count, cap, width), BF16)] * COLUMNS
        + [jax.ShapeDtypeStruct((2 * COLUMNS * cap, rows // CHUNKS), BF16)] * (count * CHUNKS),
        in_specs=[SMEM] + [VMEM] * (count * CHUNKS),
        out_specs=[VMEM] * (COLUMNS + count * CHUNKS),
        cost_estimate=pl.CostEstimate(
            flops=4 * flops, bytes_accessed=count * rows * width * 4, transcendentals=0
        ),
        name="select",
    )(where, *[close(chunk) for block in blocks for chunk in block])
    picked, mixes = outs[:COLUMNS], outs[COLUMNS:]
    return picked, [mixes[i * CHUNKS : (i + 1) * CHUNKS] for i in range(count)]


def ffn(inputs, outs, gate, up, down):
    flops = sum(2 * 3 * value.size * gate.shape[1] for value in inputs)
    return pl.pallas_call(
        functools.partial(ffn_kernel, len(inputs)),
        out_shape=[jax.ShapeDtypeStruct(shape, F32) for shape in outs],
        in_specs=[VMEM] * len(inputs) + [pl.BlockSpec(memory_space=pl.ANY)] * 3,
        out_specs=[VMEM] * len(outs),
        scratch_shapes=[pltpu.VMEM(value.shape, value.dtype) for value in (gate, up, down)]
        + [pltpu.SemaphoreType.DMA((3,))],
        cost_estimate=pl.CostEstimate(flops=flops, bytes_accessed=6 * gate.size, transcendentals=0),
        name="ffn",
    )(*[close(value) for value in inputs], gate, up, down)


def ffn_kernel(count, *refs):
    inputs, outs = refs[:count], refs[count + 3 : -4]
    gate_ref, up_ref, down_ref, arrived = refs[-4:]
    weights = zip(refs[count : count + 3], (gate_ref, up_ref, down_ref))
    copies = [pltpu.make_async_copy(here, there, arrived.at[n]) for n, (here, there) in enumerate(weights)]
    for copy in copies:
        copy.start()
    width = gate_ref.shape[0]
    rows = jnp.concatenate([ref[...].reshape(-1, width) for ref in inputs], 0)
    copies[0].wait()
    gate = jnp.dot(rows, gate_ref[...], preferred_element_type=F32)
    copies[1].wait()
    up = jnp.dot(rows, up_ref[...], preferred_element_type=F32)
    hidden = (jax.nn.silu(gate) * up).astype(BF16)
    copies[2].wait()
    result = jnp.dot(hidden, down_ref[...], preferred_element_type=F32)
    size = rows.shape[0] // len(outs)
    for n, out in enumerate(outs):
        out[...] = result[n * size : (n + 1) * size].reshape(out.shape)


def join_kernel(keep_ref, came_ref, *outs):
    count = outs[0].shape[0]
    for j, out in enumerate(outs):
        part = slice(j * count, (j + 1) * count)
        out[...] = (keep_ref[part] + came_ref[part]).astype(BF16)


def join(keep, came):
    total, cap, width = keep.shape
    return pl.pallas_call(
        join_kernel,
        out_shape=[jax.ShapeDtypeStruct((total // COLUMNS, cap, width), BF16)] * COLUMNS,
        in_specs=[VMEM] * 2,
        out_specs=[VMEM] * COLUMNS,
        cost_estimate=pl.CostEstimate(flops=20 * keep.size, bytes_accessed=10 * keep.size, transcendentals=0),
        name="join",
    )(keep, close(came))


def spread_kernel(*refs):
    parts, outs = refs[:COLUMNS], refs[COLUMNS:]
    cap = parts[0].shape[1]
    for i, out in enumerate(outs):
        for n in range(2 * COLUMNS):
            out[n * cap : (n + 1) * cap] = parts[n % COLUMNS][i]


def spread(parts):
    count, cap, width = parts[0].shape
    size = COLUMNS * parts[0].size
    return pl.pallas_call(
        spread_kernel,
        out_shape=[jax.ShapeDtypeStruct((2 * COLUMNS * cap, width), BF16)] * count,
        in_specs=[VMEM] * COLUMNS,
        out_specs=[VMEM] * count,
        cost_estimate=pl.CostEstimate(flops=20 * size, bytes_accessed=6 * size, transcendentals=0),
        name="spread",
    )(*[close(value) for value in parts])


def local(tokens, routes, gates, w_gate, w_up, w_down, shared_gate, shared_up, shared_down):
    tok_count, top_count = routes.shape
    width = tokens.shape[1]
    half = width // 2
    expert_count = lax.axis_size("expert")
    depth = expert_count // COLUMNS
    steps = depth // 2
    cap = max(2, (3 * tok_count * top_count + 2 * expert_count - 1) // (2 * expert_count))
    me, core = lax.axis_index("expert"), lax.axis_index("tensor")
    turn = (me & (COLUMNS - 1)) + jnp.arange(COLUMNS, dtype=jnp.int32)
    where = (me & ~(COLUMNS - 1)) + (turn & (COLUMNS - 1))

    def ring(value, step, back):
        pairs = []
        for z in range(depth):
            for x in range(COLUMNS):
                for c in range(2):
                    shift = (1 if c == 0 else -1) * (-1 if back else 1)
                    to = (z + shift) % depth
                    pairs.append(((z * COLUMNS + x) * 2 + c, (to * COLUMNS + x) * 2 + c))
        moved = lax.ppermute(value, ("expert", "tensor"), pairs)
        return jnp.where(core == 0, moved, value) if step == 1 else moved

    def along_x(value, shift):
        pairs = [
            (z * COLUMNS + x, z * COLUMNS + (x + shift) % COLUMNS) for z in range(depth) for x in range(COLUMNS)
        ]
        return lax.ppermute(value, "expert", pairs)

    def other_core(value):
        return lax.ppermute(value, "tensor", [(0, 1), (1, 0)])

    def split(value):
        low, high = value[:, :half], value[:, half:]
        return jnp.where(core == 0, low, high), jnp.where(core == 0, high, low)

    high = lax.reduce_precision(gates, 8, 7)
    meta = [routes.astype(BF16), high.astype(BF16), (gates - high).astype(BF16)]
    spare = jnp.zeros((tok_count, META - 3 * top_count), BF16)
    payload = jnp.concatenate([tokens] + meta + [spare], axis=1)
    piece = tok_count // CHUNKS
    held = [payload[c * piece : (c + 1) * piece] for c in range(CHUNKS)]

    held = list(lax.optimization_barrier(tuple(held)))
    blocks = {}
    for k in range(1, steps + 1):
        for c in range(CHUNKS):
            held[c] = ring(held[c], k, False)
        blocks[k] = list(held)

    (shared_part,) = ffn([tokens], [tokens.shape], shared_gate, shared_up, shared_down)
    shared_keep, shared_send = split(shared_part)
    own_cols, _ = split(tokens)
    shared_came = other_core(shared_send)
    base = lax.optimization_barrier(own_cols.astype(F32) + (shared_keep + shared_came))

    mixes, values = {}, {}
    for group in GROUPS:
        picked, mix = select([blocks[k] for k in group], where, cap, width)
        own = [picked[0]]
        for j in range(1, COLUMNS):
            own.append(along_x(picked[j], j))
        other = []
        for j in range(COLUMNS):
            other.append(other_core(own[j]))
        shape = (COLUMNS * len(group), cap, width)
        keep, send = ffn(own + other, [shape, shape], w_gate[0], w_up[0], w_down[0])
        came = other_core(send)
        summed = join(keep, came)
        back = [summed[0]]
        for j in range(1, COLUMNS):
            back.append(along_x(summed[j], -j))
        rows = spread(back)
        for i, k in enumerate(group):
            mixes[k], values[k] = mix[i], rows[i]

    moving = [None] * CHUNKS
    for k in range(steps, 0, -1):
        for c in range(CHUNKS):
            total = lax.dot_general(
                mixes[k][c], values[k], (((0,), (0,)), ((), ())), preferred_element_type=F32
            )
            if moving[c] is not None:
                total += moving[c].astype(F32)
            total = total.astype(BF16)
            moving[c] = ring(total, k, True)
    kept, sent = [], []
    for c in range(CHUNKS):
        keep, send = split(moving[c])
        kept.append(keep)
        sent.append(other_core(send))
    routed = jnp.concatenate(kept, 0).astype(F32) + jnp.concatenate(sent, 0).astype(F32)
    return (base + routed).astype(BF16)


def solution(mesh):
    in_specs = (
        P(("groups", "expert"), None),
        P(("groups", "expert"), None),
        P(("groups", "expert"), None),
        P("expert", None, "tensor"),
        P("expert", None, "tensor"),
        P("expert", "tensor", None),
        P(None, "tensor"),
        P(None, "tensor"),
        P("tensor", None),
    )
    out_specs = P(("groups", "expert"), "tensor")

    return jax.shard_map(local, mesh=mesh, in_specs=in_specs, out_specs=out_specs, check_vma=False)
```
